128 devices in a mesh: dp: 1, tp: 2 (over core), sp: 64 (over z, y, x).
Axes of the slice: x: 4, y: 4, z: 4, core: 2. Of those that a mesh axis runs over, the one named last changes fastest.
Arguments:
- hidden: bfloat16 [8, 5120], P('dp')
- lengths: int32 [8], P('dp')
- k_cache: bfloat16 [8, 16384, 8, 128], P('dp', 'sp', 'tp')
- v_cache: bfloat16 [8, 16384, 8, 128], P('dp', 'sp', 'tp')
- norm_gain: bfloat16 [5120], replicated
- w_q: bfloat16 [5120, 4096], P(None, 'tp')
- w_k: bfloat16 [5120, 1024], P(None, 'tp')
- w_v: bfloat16 [5120, 1024], P(None, 'tp')
- w_o: bfloat16 [4096, 5120], P('tp')
- inv_freq: float32 [64], replicated
Outputs:
- output 1: bfloat16 [8, 5120], P('dp')
- output 2: bfloat16 [8, 16384, 8, 128], P('dp', 'sp', 'tp')
- output 3: bfloat16 [8, 16384, 8, 128], P('dp', 'sp', 'tp')
All inputs are finite; a program needn't handle non-finite values.
Results may differ from the reference program's by a relative error of at most 0.00639264.
Values sent between devices are 32-bit elements.
A program may use at most 1 GiB of HBM per device.

```python
import jax
import jax.numpy as jnp
from jax import lax

BATCH = 8
MODEL_DIM = 5120
NUM_HEADS = 32
KV_HEADS = 8
HEAD_DIM = 128
CACHE_LEN = 16384

NORM_EPS = 1e-5
ROPE_BASE = 500000.0


def setup_inputs(seed: int = 0, part: int = 0) -> dict:
    part_key = jax.random.fold_in(jax.random.key(seed), part)
    key_list = jax.random.split(part_key, 5)
    len_keys = jax.random.split(jax.random.fold_in(part_key, 3), 4)
    shared = jax.random.split(jax.random.key(seed + 1), 6)
    hidden = 0.5 * jax.random.normal(key_list[0], (BATCH, MODEL_DIM), jnp.float32)
    long_len = jax.random.randint(len_keys[0], (BATCH,), 0, CACHE_LEN)
    short_len = jax.random.randint(len_keys[1], (BATCH,), 0, 8)
    pick_short = jax.random.randint(len_keys[2], (BATCH,), 0, 4) == 0
    perm_ids = jax.random.permutation(len_keys[3], BATCH)
    lengths = jnp.where(pick_short, short_len, long_len)
    lengths = lengths.at[perm_ids[0]].set(CACHE_LEN - 1).at[perm_ids[1]].set(0).astype(jnp.int32)
    k_cache = jax.random.normal(key_list[1], (BATCH, CACHE_LEN, KV_HEADS, HEAD_DIM), jnp.float32)
    seg_count = 64
    seg_ids = jnp.arange(CACHE_LEN) * seg_count // CACHE_LEN
    seg_means = jax.random.normal(key_list[2], (BATCH, seg_count, KV_HEADS, HEAD_DIM), jnp.float32)
    v_noise = jax.random.normal(key_list[3], (BATCH, CACHE_LEN, KV_HEADS, HEAD_DIM), jnp.float32)
    v_cache = 3.0 * seg_means[:, seg_ids] + v_noise
    norm_gain = 1.0 + 0.3 * jax.random.normal(shared[0], (MODEL_DIM,), jnp.float32)
    w_q = jax.random.normal(shared[1], (MODEL_DIM, NUM_HEADS * HEAD_DIM), jnp.float32) * MODEL_DIM ** -0.5
    w_k = jax.random.normal(shared[2], (MODEL_DIM, KV_HEADS * HEAD_DIM), jnp.float32) * MODEL_DIM ** -0.5
    w_v = jax.random.normal(shared[3], (MODEL_DIM, KV_HEADS * HEAD_DIM), jnp.float32) * MODEL_DIM ** -0.5
    w_o = jax.random.normal(shared[4], (NUM_HEADS * HEAD_DIM, MODEL_DIM), jnp.float32) * (NUM_HEADS * HEAD_DIM) ** -0.5
    exponent = jnp.arange(0, HEAD_DIM, 2).astype(jnp.float32) / HEAD_DIM
    jitter = jnp.exp(0.2 * jax.random.uniform(shared[5], (HEAD_DIM // 2,), jnp.float32, minval=-1.0, maxval=1.0))
    inv_freq = jnp.power(ROPE_BASE, -exponent) * jitter
    return {
        'hidden': hidden.astype(jnp.bfloat16),
        'lengths': lengths,
        'k_cache': k_cache.astype(jnp.bfloat16),
        'v_cache': v_cache.astype(jnp.bfloat16),
        'norm_gain': norm_gain.astype(jnp.bfloat16),
        'w_q': w_q.astype(jnp.bfloat16),
        'w_k': w_k.astype(jnp.bfloat16),
        'w_v': w_v.astype(jnp.bfloat16),
        'w_o': w_o.astype(jnp.bfloat16),
        'inv_freq': inv_freq.astype(jnp.float32),
    }


def rms_norm(hidden, norm_gain):
    hidden_f32 = hidden.astype(jnp.float32)
    inv_rms = lax.rsqrt(jnp.mean(hidden_f32 * hidden_f32, axis=-1, keepdims=True) + NORM_EPS)
    return (hidden_f32 * inv_rms * norm_gain.astype(jnp.float32)).astype(jnp.bfloat16)


def apply_rope(head_vec, angles):
    half_dim = head_vec.shape[-1] // 2
    vec_f32 = head_vec.astype(jnp.float32)
    cos_ang = jnp.cos(angles)[:, None, :]
    sin_ang = jnp.sin(angles)[:, None, :]
    lo_half = vec_f32[..., :half_dim]
    hi_half = vec_f32[..., half_dim:]
    rotated = jnp.concatenate([lo_half * cos_ang - hi_half * sin_ang, hi_half * cos_ang + lo_half * sin_ang], axis=-1)
    return rotated.astype(jnp.bfloat16)


def reference(hidden, lengths, k_cache, v_cache, norm_gain, w_q, w_k, w_v, w_o, inv_freq):
    normed = rms_norm(hidden, norm_gain)
    q_heads = jnp.dot(normed, w_q, preferred_element_type=jnp.float32).astype(jnp.bfloat16).reshape(BATCH, NUM_HEADS, HEAD_DIM)
    k_new = jnp.dot(normed, w_k, preferred_element_type=jnp.float32).astype(jnp.bfloat16).reshape(BATCH, KV_HEADS, HEAD_DIM)
    v_new = jnp.dot(normed, w_v, preferred_element_type=jnp.float32).astype(jnp.bfloat16).reshape(BATCH, KV_HEADS, HEAD_DIM)
    angles = lengths.astype(jnp.float32)[:, None] * inv_freq[None, :]
    q_rot = apply_rope(q_heads, angles)
    k_rot = apply_rope(k_new, angles)
    row_ids = jnp.arange(BATCH)
    k_out = k_cache.at[row_ids, lengths].set(k_rot)
    v_out = v_cache.at[row_ids, lengths].set(v_new)
    group_size = NUM_HEADS // KV_HEADS
    q_grp = q_rot.reshape(BATCH, KV_HEADS, group_size, HEAD_DIM)
    score_scale = HEAD_DIM ** -0.5

    def one_seq(seq_args):
        q_one, k_one, v_one, len_one = seq_args
        scores = jnp.einsum('kgd,skd->kgs', q_one.astype(jnp.float32), k_one.astype(jnp.float32)) * score_scale
        valid_mask = jnp.arange(CACHE_LEN) <= len_one
        scores = jnp.where(valid_mask, scores, -jnp.inf)
        top_score = jnp.max(scores, axis=-1, keepdims=True)
        weights = jnp.where(valid_mask, jnp.exp(scores - top_score), 0.0)
        weight_sum = jnp.sum(weights, axis=-1)
        weighted = jnp.einsum('kgs,skd->kgd', weights.astype(jnp.bfloat16).astype(jnp.float32), v_one.astype(jnp.float32))
        return (weighted / weight_sum[..., None]).astype(jnp.bfloat16)

    attn_out = lax.map(one_seq, (q_grp, k_out, v_out, lengths))
    attn_flat = attn_out.reshape(BATCH, NUM_HEADS * HEAD_DIM)
    proj_out = jnp.dot(attn_flat, w_o, preferred_element_type=jnp.float32)
    y_out = (hidden.astype(jnp.float32) + proj_out).astype(jnp.bfloat16)
    return (y_out, k_out, v_out)
```

```python
import functools

import jax
import jax.numpy as jnp
from jax import lax
from jax.experimental import pallas as pl
from jax.experimental.pallas import tpu as pltpu
from jax.sharding import PartitionSpec as P

MESH = pl.DeviceIdType.MESH
ANY = pl.BlockSpec(memory_space=pltpu.HBM)
VMEM = pl.BlockSpec(memory_space=pltpu.VMEM)
SMEM = pl.BlockSpec(memory_space=pltpu.SMEM)

NORM_EPS = 1e-5
NEG_BIG = -1e30
SIDE = 4
VMEM_LIMIT = 58 << 20
CHUNK = 1024


def coords(me):
    return lax.rem(me, SIDE), lax.rem(me // SIDE, SIDE), me // (SIDE * SIDE)


def torus_offsets():
    hops = lambda t: min(t, SIDE - t)
    all_offs = [(a, b, c) for a in range(SIDE) for b in range(SIDE) for c in range(SIDE) if a + b + c]
    return sorted(all_offs, key=lambda t: -(hops(t[0]) + hops(t[1]) + hops(t[2])))


def rope(vec, cos_full, sin_full):
    return vec * cos_full + pltpu.roll(vec, 64, 1) * sin_full


def bf16_round(val):
    return val.astype(jnp.bfloat16).astype(jnp.float32)


def decode_kernel(x_hbm, len_hbm, gain_hbm, wq_hbm, wk_hbm, wv_hbm, wo_hbm, freq_hbm, kc_hbm, vc_hbm, y_ref, k_ref, v_ref,
                  x_buf, gain_buf, freq_buf, len_buf, normed, wq_buf, wkv_buf, wo_buf, pieces, q_buf, k_new, v_new, new_score,
                  send, recv, heads, total, other,
                  small_sem, wq_sem, wkv_sem, cache_sem, wo_sem, piece_sems, part_sems, head_send_sem, head_sem, tp_sems):
    me = lax.axis_index('sp')
    tp = lax.axis_index('tp')
    x, y, z = coords(me)
    xs = [lax.rem(x + d, SIDE) for d in range(SIDE)]
    ys = [SIDE * lax.rem(y + d, SIDE) for d in range(SIDE)]
    zs = [SIDE * SIDE * lax.rem(z + d, SIDE) for d in range(SIDE)]
    sp_ids = [zs[c] + ys[b] + xs[a] for a, b, c in torus_offsets()]
    px, py, pz = lax.rem(x, 2), lax.rem(y, 2), lax.rem(z, 2)
    cx, cy, cz = x // 2, y // 2, z // 2
    my_member = px + 2 * py + 4 * pz
    my_cube = cx + 2 * cy + 4 * cz
    cube_peers = []
    for mask in range(1, 8):
        step = (mask % 2) * (1 - 2 * px) + (mask // 2 % 2) * SIDE * (1 - 2 * py) + (mask // 4) * SIDE * SIDE * (1 - 2 * pz)
        cube_peers.append(me + step)

    small = [pltpu.make_async_copy(src, dst, small_sem.at[i])
             for i, (src, dst) in enumerate([(x_hbm, x_buf), (gain_hbm, gain_buf), (freq_hbm, freq_buf), (len_hbm, len_buf)])]
    for copy in small:
        copy.start()
    steps = wq_hbm.shape[0] // CHUNK
    q_col = pl.ds(pl.multiple_of(my_member * 256, 256), 256)
    kv_col = pl.ds(pl.multiple_of(lax.rem(my_member, 4) * 128, 128), 128)
    for i in range(steps):
        rows = pl.ds(i * CHUNK, CHUNK)
        pltpu.make_async_copy(wq_hbm.at[rows, q_col], wq_buf.at[rows], wq_sem.at[i]).start()

        @pl.when(my_member < 4)
        def _():
            pltpu.make_async_copy(wk_hbm.at[rows, kv_col], wkv_buf.at[rows], wkv_sem.at[i]).start()

        @pl.when(my_member >= 4)
        def _():
            pltpu.make_async_copy(wv_hbm.at[rows, kv_col], wkv_buf.at[rows], wkv_sem.at[i]).start()

    barrier = pltpu.get_barrier_semaphore()
    for peer in sp_ids:
        pl.semaphore_signal(barrier, inc=1, device_id={'sp': peer}, device_id_type=MESH)
    pl.semaphore_signal(barrier, inc=1, device_id={'tp': 1 - tp}, device_id_type=MESH)

    caches = [pltpu.make_async_copy(kc_hbm, k_ref, cache_sem.at[0]), pltpu.make_async_copy(vc_hbm, v_ref, cache_sem.at[1])]
    for copy in caches:
        copy.start()

    def cube_at(i):
        mask = i + jnp.where(i == 3, 1, 0) - jnp.where(i == 4, 1, 0)
        a, b, c = lax.rem(mask, 2), lax.rem(mask // 2, 2), mask // 4
        return my_cube + a * (1 - 2 * cx) + 2 * b * (1 - 2 * cy) + 4 * c * (1 - 2 * cz)

    def wo_copy(i):
        rows = pl.ds(pl.multiple_of(cube_at(i) * 256, 256), 256)
        return pltpu.make_async_copy(wo_hbm.at[rows], wo_buf.at[i], wo_sem.at[i])

    def start_wo(i, carry):
        wo_copy(i).start()
        return carry

    lax.fori_loop(0, 8, start_wo, 0)

    small[0].wait()
    width = x_buf.shape[1]
    square_sum = jnp.zeros((8, 128), jnp.float32)
    for c in range(width // 128):
        val = x_buf[:, c * 128:(c + 1) * 128].astype(jnp.float32)
        square_sum = square_sum + val * val
    inv_rms = lax.rsqrt(jnp.sum(square_sum, axis=1, keepdims=True) / width + NORM_EPS)
    small[1].wait()
    for c in range(width // 128):
        val = x_buf[:, c * 128:(c + 1) * 128].astype(jnp.float32)
        normed[:, c * 128:(c + 1) * 128] = (val * inv_rms * gain_buf[c:c + 1, :].astype(jnp.float32)).astype(jnp.bfloat16)
    small[2].wait()
    small[3].wait()
    row_ids = lax.broadcasted_iota(jnp.int32, (8, 64), 0)
    pos = jnp.zeros((8, 64), jnp.int32)
    for b in range(8):
        pos = jnp.where(row_ids == b, len_buf[b], pos)
    angles = pos.astype(jnp.float32) * freq_buf[...]
    cos_ang, sin_ang = jnp.cos(angles), jnp.sin(angles)
    cos_full = jnp.concatenate([cos_ang, cos_ang], axis=1)
    sin_full = jnp.concatenate([-sin_ang, sin_ang], axis=1)
    acc_q = jnp.zeros((8, 256), jnp.float32)
    acc_kv = jnp.zeros((8, 128), jnp.float32)
    for i in range(steps):
        rows = pl.ds(i * CHUNK, CHUNK)
        lhs = normed[:, i * CHUNK:(i + 1) * CHUNK]
        pltpu.make_async_copy(wq_hbm.at[rows, q_col], wq_buf.at[rows], wq_sem.at[i]).wait()
        acc_q = acc_q + jnp.dot(lhs, wq_buf[i * CHUNK:(i + 1) * CHUNK, :], preferred_element_type=jnp.float32)
        pltpu.make_async_copy(wk_hbm.at[rows, kv_col], wkv_buf.at[rows], wkv_sem.at[i]).wait()
        acc_kv = acc_kv + jnp.dot(lhs, wkv_buf[i * CHUNK:(i + 1) * CHUNK, :], preferred_element_type=jnp.float32)
    acc_q, acc_kv = bf16_round(acc_q), bf16_round(acc_kv)
    pieces[my_member, 0] = bf16_round(rope(acc_q[:, :128], cos_full, sin_full))
    pieces[my_member, 1] = bf16_round(rope(acc_q[:, 128:], cos_full, sin_full))
    pieces[my_member, 2] = jnp.where(my_member < 4, bf16_round(rope(acc_kv, cos_full, sin_full)), acc_kv)

    pl.semaphore_wait(barrier, len(sp_ids) + 1)
    for peer in cube_peers:
        pltpu.make_async_remote_copy(pieces.at[my_member], pieces.at[my_member], piece_sems.at[0], piece_sems.at[1],
                                     device_id={'sp': peer}, device_id_type=MESH).start()
    seven = pieces.at[pl.ds(0, 7)]
    pltpu.make_async_copy(seven, seven, piece_sems.at[1]).wait()
    for j in range(8):
        q_buf[j * 16:j * 16 + 8, :] = pieces[j, 0]
        q_buf[j * 16 + 8:j * 16 + 16, :] = pieces[j, 1]
    for h in range(16):
        new_score[h * 8:h * 8 + 8, :] = jnp.broadcast_to(
            jnp.sum(q_buf[h * 8:h * 8 + 8, :] * pieces[h // 4, 2], axis=1, keepdims=True) * 128 ** -0.5, (8, 128))
        v_new[h * 8:h * 8 + 8, :] = pieces[4 + h // 4, 2]
    for j in range(4):
        k_new[j * 8:j * 8 + 8, :] = pieces[j, 2]

    for copy in caches:
        copy.wait()
    slots = k_ref.shape[0] // 32
    lanes = lax.broadcasted_iota(jnp.int32, (16, slots * 4), 1)
    head_ids = lax.broadcasted_iota(jnp.int32, (16, slots * 4), 0)
    same_head = lax.rem(lanes, 4) == head_ids // 4
    slot_ids = me * slots + lanes // 4

    def one_batch(b, carry):
        rows = pl.ds(pl.multiple_of(b * slots * 4, slots * 4), slots * 4)
        every = pl.ds(b, 16, stride=8)
        q = q_buf[every, :].astype(jnp.bfloat16)
        scores = lax.dot_general(q, k_ref[rows, :], (((1,), (1,)), ((), ())), preferred_element_type=jnp.float32) * 128 ** -0.5
        valid = same_head & (slot_ids < len_buf[b])
        local = jnp.zeros((16, 1), jnp.int32) + (len_buf[b] - me * slots)
        owned = (local >= 0) & (local < slots)
        last = jnp.where(owned, new_score[every, :][:, :1], NEG_BIG)
        scores = jnp.where(valid, scores, NEG_BIG)
        top = jnp.maximum(jnp.max(scores, axis=1, keepdims=True), last)
        weights = jnp.where(valid, jnp.exp(scores - top), 0.0)
        last_weight = jnp.where(owned, jnp.exp(last - top), 0.0)
        weight_sum = jnp.sum(weights, axis=1, keepdims=True) + last_weight
        out = jnp.dot(weights.astype(jnp.bfloat16), v_ref[rows, :], preferred_element_type=jnp.float32)
        out = out + bf16_round(last_weight) * v_new[every, :]
        some = weight_sum > 0.0
        safe = jnp.where(some, weight_sum, 1.0)
        out = jnp.where(some, out / safe, 0.0)
        log_sum = jnp.broadcast_to(jnp.where(some, top + jnp.log(safe), NEG_BIG), (16, 128))
        for pair in range(8):
            send[b * 8 + pair, 0:2, :] = out[2 * pair:2 * pair + 2]
            send[b * 8 + pair, 2:4, :] = log_sum[2 * pair:2 * pair + 2]
        return carry

    lax.fori_loop(0, 8, one_batch, 0)

    def cube_of(peer):
        u, v, w = coords(peer)
        return u // 2 + 2 * (v // 2) + 4 * (w // 2)

    def member_of(peer):
        u, v, w = coords(peer)
        return lax.rem(u, 2) + 2 * lax.rem(v, 2) + 4 * lax.rem(w, 2)

    for peer in sp_ids:
        pltpu.make_async_remote_copy(send.at[member_of(peer) * 8 + cube_of(peer)], recv.at[me], part_sems.at[0], part_sems.at[1],
                                     device_id={'sp': peer}, device_id_type=MESH).start()
    recv[me] = send[my_member * 8 + my_cube]

    tile_slots = lax.broadcasted_iota(jnp.int32, (16, 128), 0) // 4

    def update(b, carry):
        local = len_buf[b] - me * slots
        news = [jnp.concatenate([new] * 4, axis=0).astype(jnp.bfloat16)
                for new in (k_new[pl.ds(b, 4, stride=8), :], v_new[pl.ds(b, 4, stride=32), :])]

        def put(i, carry):
            for j in range(8):
                at = pl.ds(pl.multiple_of((b * (slots // 4) + i * 8 + j) * 16, 16), 16)
                hit = tile_slots + (i * 8 + j) * 4 == local
                k_ref[at, :] = jnp.where(hit, news[0], k_ref[at, :])
                v_ref[at, :] = jnp.where(hit, news[1], v_ref[at, :])
            return carry

        lax.fori_loop(0, slots // 32, put, 0)
        return carry

    lax.fori_loop(0, 8, update, 0)

    most = recv.at[pl.ds(0, 63)]
    pltpu.make_async_copy(most, most, part_sems.at[1]).wait()
    best = recv[0, 2:4, :]
    for i in range(1, 64):
        best = jnp.maximum(best, recv[i, 2:4, :])
    weighted = jnp.zeros((2, 128), jnp.float32)
    factor_sum = jnp.zeros((2, 128), jnp.float32)
    for i in range(64):
        factor = jnp.exp(recv[i, 2:4, :] - best)
        weighted = weighted + factor * recv[i, 0:2, :]
        factor_sum = factor_sum + factor
    heads[my_cube, my_member] = bf16_round(weighted / factor_sum)

    for peer in sp_ids:
        pltpu.make_async_remote_copy(heads.at[my_cube, my_member], heads.at[my_cube, my_member], head_send_sem, head_sem.at[my_cube],
                                     device_id={'sp': peer}, device_id_type=MESH).start()
    total[...] = jnp.zeros_like(total)

    def one_block(i, carry):
        cube = cube_at(i)

        @pl.when(i == 0)
        def _():
            members = heads.at[cube, pl.ds(0, 7)]
            pltpu.make_async_copy(members, members, head_sem.at[cube]).wait()

        @pl.when(i > 0)
        def _():
            pltpu.make_async_copy(heads.at[cube], heads.at[cube], head_sem.at[cube]).wait()

        wo_copy(i).wait()
        lhs = jnp.concatenate([heads[cube, :, 0, :], heads[cube, :, 1, :]], axis=1).astype(jnp.bfloat16)
        total[...] += jnp.dot(lhs, wo_buf[i], preferred_element_type=jnp.float32)
        return carry

    lax.fori_loop(0, 8, one_block, 0)

    swap = pltpu.make_async_remote_copy(total, other, tp_sems.at[0], tp_sems.at[1], device_id={'tp': 1 - tp}, device_id_type=MESH)
    swap.start()
    pltpu.make_async_copy(seven, seven, piece_sems.at[0]).wait()
    pltpu.make_async_copy(most, most, part_sems.at[0]).wait()
    sent = heads.at[pl.ds(0, 7)]
    pltpu.make_async_copy(sent, sent, head_send_sem).wait()
    sent = heads.at[0, pl.ds(0, 7)]
    pltpu.make_async_copy(sent, sent, head_send_sem).wait()
    swap.wait()
    y_ref[...] = (x_buf[...].astype(jnp.float32) + (total[...] + other[...])).astype(jnp.bfloat16)


def device_step(hidden, lengths, k_cache, v_cache, norm_gain, w_q, w_k, w_v, w_o, inv_freq):
    batch, width = hidden.shape
    f32, bf16 = jnp.float32, jnp.bfloat16
    dma = pltpu.SemaphoreType.DMA
    steps = width // CHUNK
    rows = k_cache.shape[0] * k_cache.shape[1] * k_cache.shape[2]
    flat = jax.ShapeDtypeStruct((rows, 128), bf16)
    y_out, k_upd, v_upd = pl.pallas_call(
        decode_kernel,
        out_shape=[jax.ShapeDtypeStruct((batch, width), bf16), flat, flat],
        in_specs=[ANY] * 10,
        out_specs=[VMEM] * 3,
        scratch_shapes=[
            pltpu.VMEM((batch, width), bf16), pltpu.VMEM((width // 128, 128), bf16), pltpu.VMEM((1, 64), f32), pltpu.SMEM((batch,), jnp.int32),
            pltpu.VMEM((batch, width), bf16), pltpu.VMEM((width, 256), bf16), pltpu.VMEM((width, 128), bf16), pltpu.VMEM((8, 256, width), bf16),
            pltpu.VMEM((8, 3, 8, 128), f32), pltpu.VMEM((128, 128), f32), pltpu.VMEM((32, 128), f32), pltpu.VMEM((128, 128), f32),
            pltpu.VMEM((128, 128), f32), pltpu.VMEM((64, 4, 128), f32), pltpu.VMEM((64, 4, 128), f32), pltpu.VMEM((8, 8, 2, 128), f32),
            pltpu.VMEM((batch, width), f32), pltpu.VMEM((batch, width), f32),
            dma((4,)), dma((steps,)), dma((steps,)), dma((2,)), dma((8,)), dma((2,)), dma((2,)), dma, dma((8,)), dma((2,)),
        ],
        compiler_params=pltpu.CompilerParams(collective_id=0, has_side_effects=True, vmem_limit_bytes=VMEM_LIMIT),
        name='decode',
    )(hidden, lengths, norm_gain.reshape(width // 128, 128), w_q, w_k, w_v, w_o, inv_freq.reshape(1, 64),
      k_cache.reshape(rows, 128), v_cache.reshape(rows, 128))
    return y_out, k_upd.reshape(k_cache.shape), v_upd.reshape(v_cache.shape)


def solution(mesh):
    cache_spec = P('dp', 'sp', 'tp', None)
    in_specs = (P('dp', None), P('dp'), cache_spec, cache_spec, P(None), P(None, 'tp'), P(None, 'tp'), P(None, 'tp'), P('tp', None), P(None))
    out_specs = (P('dp', None), cache_spec, cache_spec)
    return jax.shard_map(device_step, mesh=mesh, in_specs=in_specs, out_specs=out_specs, check_vma=False)
```

```python
import functools

import jax
import jax.numpy as jnp
from jax import lax
from jax.experimental import pallas as pl
from jax.experimental.pallas import tpu as pltpu
from jax.sharding import PartitionSpec as P

MESH = pl.DeviceIdType.MESH
ANY = pl.BlockSpec(memory_space=pltpu.HBM)
VMEM = pl.BlockSpec(memory_space=pltpu.VMEM)
SMEM = pl.BlockSpec(memory_space=pltpu.SMEM)

NORM_EPS = 1e-5
NEG_BIG = -1e30
SIDE = 4
VMEM_LIMIT = 59 << 20
GROUP = 4
CHUNK = 1024


def coords(me):
    return lax.rem(me, SIDE), lax.rem(me // SIDE, SIDE), me // (SIDE * SIDE)


def torus_offsets():
    hops = lambda t: min(t, SIDE - t)
    all_offs = [(a, b, c) for a in range(SIDE) for b in range(SIDE) for c in range(SIDE) if a + b + c]
    return sorted(all_offs, key=lambda t: -(hops(t[0]) + hops(t[1]) + hops(t[2])))


def rope(vec, cos_full, sin_full):
    return vec * cos_full + pltpu.roll(vec, 64, 1) * sin_full


def bf16_round(val):
    return val.astype(jnp.bfloat16).astype(jnp.float32)


def decode_kernel(x_hbm, len_hbm, gain_hbm, wq_hbm, wk_hbm, wv_hbm, wo_hbm, freq_hbm, kc_hbm, vc_hbm, y_ref, k_ref, v_ref,
                  x_buf, gain_buf, freq_buf, len_buf, normed, wq_buf, wkv_buf, wo_buf, pieces, q_buf, k_new, v_new, new_score,
                  send_lo, send_hi, recv, heads, total, other,
                  small_sem, wq_sem, wkv_sem, cache_sem, wo_sem, piece_sems, part_sems, head_send_sem, head_sem, tp_sems):
    me = lax.axis_index('sp')
    tp = lax.axis_index('tp')
    x, y, z = coords(me)
    xs = [lax.rem(x + d, SIDE) for d in range(SIDE)]
    ys = [SIDE * lax.rem(y + d, SIDE) for d in range(SIDE)]
    zs = [SIDE * SIDE * lax.rem(z + d, SIDE) for d in range(SIDE)]
    sp_ids = [zs[c] + ys[b] + xs[a] for a, b, c in torus_offsets()]
    px, py, pz = lax.rem(x, 2), lax.rem(y, 2), lax.rem(z, 2)
    cx, cy, cz = x // 2, y // 2, z // 2
    my_member = px + 2 * py + 4 * pz
    my_cube = cx + 2 * cy + 4 * cz
    cube_peers = []
    for mask in range(1, 8):
        step = (mask % 2) * (1 - 2 * px) + (mask // 2 % 2) * SIDE * (1 - 2 * py) + (mask // 4) * SIDE * SIDE * (1 - 2 * pz)
        cube_peers.append(me + step)

    small = [pltpu.make_async_copy(src, dst, small_sem.at[i])
             for i, (src, dst) in enumerate([(x_hbm, x_buf), (gain_hbm, gain_buf), (freq_hbm, freq_buf), (len_hbm, len_buf)])]
    for i in (3, 2, 0, 1):
        small[i].start()
    steps = wq_hbm.shape[0] // CHUNK
    q_col = pl.ds(pl.multiple_of(my_member * 256, 256), 256)
    kv_col = pl.ds(pl.multiple_of(lax.rem(my_member, 4) * 128, 128), 128)
    for i in range(steps):
        rows = pl.ds(i * CHUNK, CHUNK)
        pltpu.make_async_copy(wq_hbm.at[rows, q_col], wq_buf.at[rows], wq_sem.at[i]).start()

        @pl.when(my_member < 4)
        def _():
            pltpu.make_async_copy(wk_hbm.at[rows, kv_col], wkv_buf.at[rows], wkv_sem.at[i]).start()

        @pl.when(my_member >= 4)
        def _():
            pltpu.make_async_copy(wv_hbm.at[rows, kv_col], wkv_buf.at[rows], wkv_sem.at[i]).start()

    barrier = pltpu.get_barrier_semaphore()
    for peer in sp_ids:
        pl.semaphore_signal(barrier, inc=1, device_id={'sp': peer}, device_id_type=MESH)
    pl.semaphore_signal(barrier, inc=1, device_id={'tp': 1 - tp}, device_id_type=MESH)

    def cube_at(i):
        mask = i + jnp.where(i == 3, 1, 0) - jnp.where(i == 4, 1, 0)
        a, b, c = lax.rem(mask, 2), lax.rem(mask // 2, 2), mask // 4
        return my_cube + a * (1 - 2 * cx) + 2 * b * (1 - 2 * cy) + 4 * c * (1 - 2 * cz)

    def wo_copy(i):
        rows = pl.ds(pl.multiple_of(cube_at(i) * 256, 256), 256)
        return pltpu.make_async_copy(wo_hbm.at[rows], wo_buf.at[i], wo_sem.at[i])

    def start_wo(i, carry):
        wo_copy(i).start()
        return carry

    small[2].wait()
    small[3].wait()
    row_ids = lax.broadcasted_iota(jnp.int32, (8, 64), 0)
    pos = jnp.zeros((8, 64), jnp.int32)
    for b in range(8):
        pos = jnp.where(row_ids == b, len_buf[b], pos)
    angles = pos.astype(jnp.float32) * freq_buf[...]
    cos_ang, sin_ang = jnp.cos(angles), jnp.sin(angles)
    cos_full = jnp.concatenate([cos_ang, cos_ang], axis=1)
    sin_full = jnp.concatenate([-sin_ang, sin_ang], axis=1)
    small[0].wait()
    width = x_buf.shape[1]
    square_sum = jnp.zeros((8, 128), jnp.float32)
    for c in range(width // 128):
        val = x_buf[:, c * 128:(c + 1) * 128].astype(jnp.float32)
        square_sum = square_sum + val * val
    inv_rms = lax.rsqrt(jnp.sum(square_sum, axis=1, keepdims=True) / width + NORM_EPS)
    small[1].wait()
    for c in range(width // 128):
        val = x_buf[:, c * 128:(c + 1) * 128].astype(jnp.float32)
        normed[:, c * 128:(c + 1) * 128] = (val * inv_rms * gain_buf[c:c + 1, :].astype(jnp.float32)).astype(jnp.bfloat16)
    acc_q = jnp.zeros((8, 256), jnp.float32)
    acc_kv = jnp.zeros((8, 128), jnp.float32)
    for i in range(steps):
        rows = pl.ds(i * CHUNK, CHUNK)
        lhs = normed[:, i * CHUNK:(i + 1) * CHUNK]
        pltpu.make_async_copy(wq_hbm.at[rows, q_col], wq_buf.at[rows], wq_sem.at[i]).wait()
        acc_q = acc_q + jnp.dot(lhs, wq_buf[i * CHUNK:(i + 1) * CHUNK, :], preferred_element_type=jnp.float32)
        pltpu.make_async_copy(wk_hbm.at[rows, kv_col], wkv_buf.at[rows], wkv_sem.at[i]).wait()
        acc_kv = acc_kv + jnp.dot(lhs, wkv_buf[i * CHUNK:(i + 1) * CHUNK, :], preferred_element_type=jnp.float32)
    caches = [pltpu.make_async_copy(kc_hbm, k_ref, cache_sem.at[0]), pltpu.make_async_copy(vc_hbm, v_ref, cache_sem.at[1])]
    for copy in caches:
        copy.start()
    acc_q, acc_kv = bf16_round(acc_q), bf16_round(acc_kv)
    pieces[my_member, 0] = bf16_round(rope(acc_q[:, :128], cos_full, sin_full))
    pieces[my_member, 1] = bf16_round(rope(acc_q[:, 128:], cos_full, sin_full))
    pieces[my_member, 2] = jnp.where(my_member < 4, bf16_round(rope(acc_kv, cos_full, sin_full)), acc_kv)

    pl.semaphore_wait(barrier, len(sp_ids) + 1)
    for peer in cube_peers:
        pltpu.make_async_remote_copy(pieces.at[my_member], pieces.at[my_member], piece_sems.at[0], piece_sems.at[1],
                                     device_id={'sp': peer}, device_id_type=MESH).start()
    lax.fori_loop(0, 8, start_wo, 0)
    seven = pieces.at[pl.ds(0, 7)]
    pltpu.make_async_copy(seven, seven, piece_sems.at[1]).wait()
    for j in range(8):
        q_buf[j * 16:j * 16 + 8, :] = pieces[j, 0]
        q_buf[j * 16 + 8:j * 16 + 16, :] = pieces[j, 1]
    for h in range(16):
        new_score[h * 8:h * 8 + 8, :] = jnp.broadcast_to(
            jnp.sum(q_buf[h * 8:h * 8 + 8, :] * pieces[h // 4, 2], axis=1, keepdims=True) * 128 ** -0.5, (8, 128))
        v_new[h * 8:h * 8 + 8, :] = pieces[4 + h // 4, 2]
    for j in range(4):
        k_new[j * 8:j * 8 + 8, :] = pieces[j, 2]

    for copy in caches:
        copy.wait()
    slots = k_ref.shape[0] // 32
    lanes = lax.broadcasted_iota(jnp.int32, (16, slots * 4), 1)
    head_ids = lax.broadcasted_iota(jnp.int32, (16, slots * 4), 0)
    same_head = lax.rem(lanes, 4) == head_ids // 4
    slot_ids = me * slots + lanes // 4

    cube_base = [2 * ((cx + a * (1 - 2 * cx)) + SIDE * (cy + b * (1 - 2 * cy)) + SIDE * SIDE * (cz + c * (1 - 2 * cz)))
                 for c in range(2) for b in range(2) for a in range(2)]
    cube_id = [my_cube + a * (1 - 2 * cx) + 2 * b * (1 - 2 * cy) + 4 * c * (1 - 2 * cz)
               for c in range(2) for b in range(2) for a in range(2)]

    def send_part(b, near):
        peer = cube_base[near] + (b % 2 + b // 2 % 2 * SIDE + b // 4 * SIDE * SIDE)
        send = send_lo if b < GROUP else send_hi
        pltpu.make_async_remote_copy(send.at[b % GROUP * 8 + cube_id[near]], recv.at[me], part_sems.at[0], part_sems.at[1],
                                     device_id={'sp': peer}, device_id_type=MESH).start()

    for first in range(0, 8, GROUP):
        group = range(first, first + GROUP)
        send = send_lo if first < GROUP else send_hi
        scores, valid, owned, last = {}, {}, {}, {}
        for b in group:
            q = q_buf[pl.ds(b, 16, stride=8), :].astype(jnp.bfloat16)
            scores[b] = lax.dot_general(q, k_ref[b * slots * 4:(b + 1) * slots * 4, :], (((1,), (1,)), ((), ())),
                                        preferred_element_type=jnp.float32) * 128 ** -0.5
        for b in group:
            valid[b] = same_head & (slot_ids < len_buf[b])
            local = jnp.zeros((16, 1), jnp.int32) + (len_buf[b] - me * slots)
            owned[b] = (local >= 0) & (local < slots)
            last[b] = jnp.where(owned[b], new_score[pl.ds(b, 16, stride=8), :][:, :1], NEG_BIG)
            scores[b] = jnp.where(valid[b], scores[b], NEG_BIG)
        for b in group:
            top = jnp.maximum(jnp.max(scores[b], axis=1, keepdims=True), last[b])
            weights = jnp.where(valid[b], jnp.exp(scores[b] - top), 0.0)
            last_weight = jnp.where(owned[b], jnp.exp(last[b] - top), 0.0)
            weight_sum = jnp.sum(weights, axis=1, keepdims=True) + last_weight
            out = jnp.dot(weights.astype(jnp.bfloat16), v_ref[b * slots * 4:(b + 1) * slots * 4, :], preferred_element_type=jnp.float32)
            out = out + bf16_round(last_weight) * v_new[pl.ds(b, 16, stride=8), :]
            some = weight_sum > 0.0
            safe = jnp.where(some, weight_sum, 1.0)
            out = jnp.where(some, out / safe, 0.0)
            log_sum = jnp.broadcast_to(jnp.where(some, top + jnp.log(safe), NEG_BIG), (16, 128))
            for pair in range(8):
                send[b % GROUP * 8 + pair, 0:2, :] = out[2 * pair:2 * pair + 2]
                send[b % GROUP * 8 + pair, 2:4, :] = log_sum[2 * pair:2 * pair + 2]
        for near in range(7, 0, -1):
            for b in group:
                send_part(b, near)
        for b in group:
            @pl.when(my_member != b)
            def _():
                send_part(b, 0)

    @pl.when(my_member < GROUP)
    def _():
        recv[me] = send_lo[my_member * 8 + my_cube]

    @pl.when(my_member >= GROUP)
    def _():
        recv[me] = send_hi[(my_member - GROUP) * 8 + my_cube]

    tile_slots = (lax.broadcasted_iota(jnp.int32, (16, 128), 0) // 4).astype(jnp.bfloat16)

    def update(b, carry):
        local = len_buf[b] - me * slots
        local = jnp.clip(local, -SIDE, slots).astype(jnp.float32)
        news = [jnp.concatenate([new] * 4, axis=0).astype(jnp.bfloat16)
                for new in (k_new[pl.ds(b, 4, stride=8), :], v_new[pl.ds(b, 4, stride=32), :])]

        def put(i, carry):
            for j in range(8):
                at = pl.ds(pl.multiple_of((b * (slots // 4) + i * 8 + j) * 16, 16), 16)
                here = jnp.broadcast_to(local - ((i * 8 + j) * 4).astype(jnp.float32), (16, 128)).astype(jnp.bfloat16)
                hit = tile_slots == here
                k_ref[at, :] = jnp.where(hit, news[0], k_ref[at, :])
                v_ref[at, :] = jnp.where(hit, news[1], v_ref[at, :])
            return carry

        lax.fori_loop(0, slots // 32, put, 0)
        return carry

    lax.fori_loop(0, 8, update, 0)

    most = recv.at[pl.ds(0, 63)]
    pltpu.make_async_copy(most, most, part_sems.at[1]).wait()
    best = recv[0, 2:4, :]
    for i in range(1, 64):
        best = jnp.maximum(best, recv[i, 2:4, :])
    weighted = jnp.zeros((2, 128), jnp.float32)
    factor_sum = jnp.zeros((2, 128), jnp.float32)
    for i in range(64):
        factor = jnp.exp(recv[i, 2:4, :] - best)
        weighted = weighted + factor * recv[i, 0:2, :]
        factor_sum = factor_sum + factor
    heads[my_cube, my_member] = bf16_round(weighted / factor_sum)

    for peer in sp_ids:
        pltpu.make_async_remote_copy(heads.at[my_cube, my_member], heads.at[my_cube, my_member], head_send_sem, head_sem.at[my_cube],
                                     device_id={'sp': peer}, device_id_type=MESH).start()
    total[...] = jnp.zeros_like(total)

    def one_block(i, carry):
        cube = cube_at(i)

        @pl.when(i == 0)
        def _():
            members = heads.at[cube, pl.ds(0, 7)]
            pltpu.make_async_copy(members, members, head_sem.at[cube]).wait()

        @pl.when(i > 0)
        def _():
            pltpu.make_async_copy(heads.at[cube], heads.at[cube], head_sem.at[cube]).wait()

        wo_copy(i).wait()
        lhs = jnp.concatenate([heads[cube, :, 0, :], heads[cube, :, 1, :]], axis=1).astype(jnp.bfloat16)
        total[...] += jnp.dot(lhs, wo_buf[i], preferred_element_type=jnp.float32)
        return carry

    lax.fori_loop(0, 8, one_block, 0)

    swap = pltpu.make_async_remote_copy(total, other, tp_sems.at[0], tp_sems.at[1], device_id={'tp': 1 - tp}, device_id_type=MESH)
    swap.start()
    pltpu.make_async_copy(seven, seven, piece_sems.at[0]).wait()
    pltpu.make_async_copy(most, most, part_sems.at[0]).wait()
    sent = heads.at[pl.ds(0, 7)]
    pltpu.make_async_copy(sent, sent, head_send_sem).wait()
    sent = heads.at[0, pl.ds(0, 7)]
    pltpu.make_async_copy(sent, sent, head_send_sem).wait()
    swap.wait()
    y_ref[...] = (x_buf[...].astype(jnp.float32) + (total[...] + other[...])).astype(jnp.bfloat16)


def finish_kernel(y_in, k_in, v_in, y_hbm, k_hbm, v_hbm, sems):
    copies = [pltpu.make_async_copy(src, dst, sems.at[i]) for i, (src, dst) in enumerate([(k_in, k_hbm), (v_in, v_hbm), (y_in, y_hbm)])]
    for copy in copies:
        copy.start()
    for copy in copies:
        copy.wait()


def device_step(hidden, lengths, k_cache, v_cache, norm_gain, w_q, w_k, w_v, w_o, inv_freq):
    batch, width = hidden.shape
    f32, bf16 = jnp.float32, jnp.bfloat16
    dma = pltpu.SemaphoreType.DMA
    steps = width // CHUNK
    rows = k_cache.shape[0] * k_cache.shape[1] * k_cache.shape[2]
    flat = jax.ShapeDtypeStruct((rows, 128), bf16)
    small = jax.ShapeDtypeStruct((batch, width), bf16)
    outs = pl.pallas_call(
        decode_kernel,
        out_shape=[pltpu.VMEM((batch, width), bf16), pltpu.VMEM((rows, 128), bf16), pltpu.VMEM((rows, 128), bf16)],
        in_specs=[ANY] * 10,
        out_specs=[VMEM] * 3,
        scratch_shapes=[
            pltpu.VMEM((batch, width), bf16), pltpu.VMEM((width // 128, 128), bf16), pltpu.VMEM((1, 64), f32), pltpu.SMEM((batch,), jnp.int32),
            pltpu.VMEM((batch, width), bf16), pltpu.VMEM((width, 256), bf16), pltpu.VMEM((width, 128), bf16), pltpu.VMEM((8, 256, width), bf16),
            pltpu.VMEM((8, 3, 8, 128), f32), pltpu.VMEM((128, 128), f32), pltpu.VMEM((32, 128), f32), pltpu.VMEM((128, 128), f32),
            pltpu.VMEM((128, 128), f32), pltpu.VMEM((32, 4, 128), f32), pltpu.VMEM((32, 4, 128), f32), pltpu.VMEM((64, 4, 128), f32), pltpu.VMEM((8, 8, 2, 128), f32),
            pltpu.VMEM((batch, width), f32), pltpu.VMEM((batch, width), f32),
            dma((4,)), dma((steps,)), dma((steps,)), dma((2,)), dma((8,)), dma((2,)), dma((2,)), dma, dma((8,)), dma((2,)),
        ],
        compiler_params=pltpu.CompilerParams(collective_id=0, has_side_effects=True, vmem_limit_bytes=VMEM_LIMIT),
        name='decode',
    )(hidden, lengths, norm_gain.reshape(width // 128, 128), w_q, w_k, w_v, w_o, inv_freq.reshape(1, 64),
      k_cache.reshape(rows, 128), v_cache.reshape(rows, 128))
    y_out, k_upd, v_upd = pl.pallas_call(
        finish_kernel,
        out_shape=[small, flat, flat],
        in_specs=[VMEM] * 3,
        out_specs=[ANY] * 3,
        scratch_shapes=[dma((3,))],
        compiler_params=pltpu.CompilerParams(vmem_limit_bytes=1 << 20),
        name='finish',
    )(*outs)
    return y_out, k_upd.reshape(k_cache.shape), v_upd.reshape(v_cache.shape)


def solution(mesh):
    cache_spec = P('dp', 'sp', 'tp', None)
    in_specs = (P('dp', None), P('dp'), cache_spec, cache_spec, P(None), P(None, 'tp'), P(None, 'tp'), P(None, 'tp'), P('tp', None), P(None))
    out_specs = (P('dp', None), cache_spec, cache_spec)
    return jax.shard_map(device_step, mesh=mesh, in_specs=in_specs, out_specs=out_specs, check_vma=False)
```
